8 devices in a mesh: dp: 2 (over y, z), ep: 4 (over x, core).
Axes of the slice: x: 2, y: 2, z: 1, core: 2. Of those that a mesh axis runs over, the one named last changes fastest.
Arguments:
- x: bfloat16 [2, 4, 768, 2048], P('dp', 'ep'), parts along dimension 0
- expert: int32 [2, 4, 768, 6], P('dp', 'ep'), parts along dimension 0
- slot: int32 [2, 4, 768, 6], P('dp', 'ep'), parts along dimension 0
- gate: float32 [2, 4, 768, 6], P('dp', 'ep'), parts along dimension 0
- w_gate: bfloat16 [64, 2048, 1408], P('ep')
- w_up: bfloat16 [64, 2048, 1408], P('ep')
- w_down: bfloat16 [64, 1408, 2048], P('ep')
- s_gate: bfloat16 [2048, 2816], replicated
- s_up: bfloat16 [2048, 2816], replicated
- s_down: bfloat16 [2816, 2048], replicated
Outputs:
- y: bfloat16 [2, 4, 768, 2048], P('dp', 'ep'), parts along dimension 0
There are 2 independent parts. The reference program is written for one: setup_inputs(seed, part) draws one part's arguments, and reference() takes and returns one part's arrays. A program takes and returns all parts, laid end to end along the dimension named above; an argument that names none is the same for every part.
All inputs are finite; a program needn't handle non-finite values.
Results may differ from the reference program's by a relative error of at most 0.009.
Values are sent between devices in bfloat16 or wider.
A program may use at most 2 GiB of HBM per device.

```python
import jax
import jax.numpy as jnp

MEMBERS = 4
TOKENS = 768
D = 2048
FF = 1408
TOP = 6
EXPERTS = 64
SHARED_FF = 2816
SLOTS = 5 * TOKENS * TOP // (4 * EXPERTS)


def setup_inputs(seed: int = 0, part: int = 0) -> dict:
    own, k1, k2, k3, k4, k5, k6 = jax.random.split(jax.random.key(seed), 7)
    kx, ke, kl, kg = jax.random.split(jax.random.fold_in(own, part), 4)
    devices = (1, MEMBERS)
    place = jax.random.permutation(kl, jnp.arange(EXPERTS, dtype=jnp.uint32))
    slow = ((EXPERTS + (9 * place) % EXPERTS) << ((9 * place) // EXPERTS)) // EXPERTS
    wait = (jax.random.bits(ke, (*devices, TOKENS, EXPERTS), jnp.uint32) >> 10) * slow
    expert = jnp.argsort(wait, axis=-1)[..., :TOP].astype(jnp.int32)
    chosen = jax.nn.one_hot(expert, EXPERTS, dtype=jnp.int32)
    in_line = jnp.cumsum(chosen.reshape(*devices, TOKENS * TOP, EXPERTS), axis=2) - 1
    slot = jnp.sum(in_line.reshape(chosen.shape) * chosen, axis=-1)

    def one(key, rows, columns):
        return (jax.random.normal(key, (rows, columns), jnp.float32) * rows**-0.5).astype(jnp.bfloat16)

    def weights(key, rows, columns):
        return jax.lax.map(lambda k: one(k, rows, columns), jax.random.split(key, EXPERTS))

    return {
        "x": jax.random.normal(kx, (*devices, TOKENS, D), jnp.float32).astype(jnp.bfloat16),
        "expert": expert,
        "slot": slot,
        "gate": jax.nn.softmax(jax.random.normal(kg, expert.shape, jnp.float32)),
        "w_gate": weights(k1, D, FF),
        "w_up": weights(k2, D, FF),
        "w_down": weights(k3, FF, D),
        "s_gate": one(k4, D, SHARED_FF),
        "s_up": one(k5, D, SHARED_FF),
        "s_down": one(k6, SHARED_FF, D),
    }


def einsum(form, a, b):
    return jnp.einsum(form, a.astype(jnp.float32), b.astype(jnp.float32))


def for_all(x, s_gate, s_up, s_down):
    h = jax.nn.silu(einsum("...d,df->...f", x, s_gate)) * einsum("...d,df->...f", x, s_up)
    return einsum("...f,fd->...d", h.astype(jnp.bfloat16), s_down)


def reference(x, expert, slot, gate, w_gate, w_up, w_down, s_gate, s_up, s_down):
    to_expert = jax.nn.one_hot(expert, EXPERTS, dtype=jnp.bfloat16)
    to_slot = jax.nn.one_hot(slot, SLOTS, dtype=jnp.bfloat16)
    weighted = to_expert * gate[..., None].astype(jnp.bfloat16)
    dispatch = einsum("abtke,abtkc->abtec", to_expert, to_slot).astype(jnp.bfloat16)
    combine = einsum("abtke,abtkc->abtec", weighted, to_slot).astype(jnp.bfloat16)
    z = einsum("abtec,abtd->aebcd", dispatch, x).astype(jnp.bfloat16)
    h = jax.nn.silu(einsum("aebcd,edf->aebcf", z, w_gate))
    h = (h * einsum("aebcd,edf->aebcf", z, w_up)).astype(jnp.bfloat16)
    out = einsum("aebcf,efd->aebcd", h, w_down).astype(jnp.bfloat16)
    y = einsum("abtec,aebcd->abtd", combine, out)
    return (y + for_all(x, s_gate, s_up, s_down)).astype(jnp.bfloat16)
```

```python
import functools

import jax
import jax.numpy as jnp
from jax import lax
from jax.experimental import pallas as pl
from jax.experimental.pallas import tpu as pltpu
from jax.sharding import PartitionSpec as P


F32, BF16, I32 = jnp.float32, jnp.bfloat16, jnp.int32
VMEM = 66_000_000
GROUP, BLOCK, STRIDE, PIECE, TILE = 16, 256, 128, 32, 128
CHUNKS = 4


def dot(a, b):
    return jnp.dot(a, b, preferred_element_type=F32)


def params():
    return pltpu.CompilerParams(vmem_limit_bytes=VMEM)


def cost(flops, nbytes):
    return pl.CostEstimate(flops=int(flops), bytes_accessed=int(nbytes), transcendentals=0)


def whole(v):
    return pl.BlockSpec(v.shape, lambda *_: (0,) * v.ndim, pipeline_mode=pl.Buffered(1))


def aligned(v, m=GROUP):
    return pl.multiple_of(v, m)


def route_kernel(local, me_ref, *refs):
    infos, (pos_ref, table_ref) = refs[:4], refs[4:]
    top, tokens = pos_ref.shape[1:]
    expert = lax.broadcasted_iota(I32, (local, tokens), 0)
    a = lax.broadcasted_iota(I32, (local, STRIDE), 0)
    b = lax.broadcasted_iota(I32, (local, STRIDE), 1)
    for s, info in enumerate(infos):
        code = info[:top, :].astype(I32) - me_ref[0] * (local * STRIDE)
        mine = (code >= 0) & (code < local * STRIDE)
        which = jnp.where(mine, lax.shift_right_logical(code, 7), -1)
        place = jnp.where(mine, code & (STRIDE - 1), 0)
        most = jnp.zeros((local, tokens), I32)
        for j in range(top):
            most = jnp.maximum(most, jnp.where(which[j : j + 1] == expert, place[j : j + 1] + 1, 0))
        used = jnp.max(most.astype(F32), axis=1, keepdims=True).astype(I32)
        used = (used + (GROUP - 1)) & ~(GROUP - 1)
        as_row = lambda m: jnp.sum(jnp.where(m, used.astype(F32), 0.0), axis=0, keepdims=True)
        row, start_row = as_row(a == b), as_row(a < b)
        start = jnp.sum(jnp.where((b < a) & (b < local), row, 0.0), axis=1, keepdims=True).astype(I32)
        for j in range(top):
            at = jnp.sum(jnp.where(which[j : j + 1] == expert, start, 0).astype(F32), axis=0, keepdims=True).astype(I32)
            pos_ref[s, j : j + 1, :] = jnp.where(mine[j : j + 1], at + place[j : j + 1], -1)
        table_ref[s : s + 1, :] = row.astype(I32)
        table_ref[4 + s : 5 + s, :] = start_row.astype(I32)


def route(me, infos, local, top):
    tokens = infos[0].shape[1]
    return pl.pallas_call(
        functools.partial(route_kernel, local),
        in_specs=[pl.BlockSpec(memory_space=pltpu.SMEM)] + [pl.BlockSpec(memory_space=pltpu.VMEM)] * 4,
        out_specs=[pl.BlockSpec(memory_space=pltpu.VMEM)] * 2,
        out_shape=[jax.ShapeDtypeStruct((4, top, tokens), I32), jax.ShapeDtypeStruct((8, STRIDE), I32)],
        cost_estimate=cost(1e9, 1e6),
        name="route",
    )(me, *infos)


def gather_kernel(s, local, table_ref, pos_ref, info_ref, x_ref, z_ref, c_ref):
    i, (top, tokens) = pl.program_id(0), pos_ref.shape[1:]

    @pl.when(i * BLOCK < table_ref[4 + s, local])
    def _():
        row = lax.broadcasted_iota(I32, (BLOCK, tokens), 0) + i * BLOCK
        c, one = jnp.zeros((BLOCK, tokens), F32), jnp.zeros((BLOCK, tokens), F32)
        for j in range(top):
            hit = pos_ref[s, j : j + 1, :] == row
            c = jnp.where(hit, info_ref[top + j : top + j + 1, :], c)
            one = jnp.where(hit, 1.0, one)
        z_ref[...] = dot(one.astype(BF16), x_ref[...]).astype(BF16)
        c_ref[...] = c.T.astype(BF16)


def gather(table, pos, info, x, rows, s, local):
    tokens, d = x.shape
    last = lambda i, t: jnp.minimum(i, jnp.maximum((t[4 + s, local] + (BLOCK - 1)) // BLOCK - 1, 0))
    return pl.pallas_call(
        functools.partial(gather_kernel, s, local),
        grid_spec=pltpu.PrefetchScalarGridSpec(
            num_scalar_prefetch=1,
            grid=(rows // BLOCK,),
            in_specs=[whole(pos), whole(info), whole(x)],
            out_specs=[
                pl.BlockSpec((BLOCK, d), lambda i, t: (last(i, t), 0)),
                pl.BlockSpec((tokens, BLOCK), lambda i, t: (0, last(i, t))),
            ],
        ),
        out_shape=[jax.ShapeDtypeStruct((rows, d), BF16), jax.ShapeDtypeStruct((tokens, rows), BF16)],
        compiler_params=params(),
        cost_estimate=cost(2 * rows * tokens * d, 2 * rows * (tokens + d)),
        name="gather",
    )(table, pos, info, x)


def by_rows(total, most, body):
    for m in range(TILE, most + TILE, TILE):
        pl.when((total > m - TILE) & (total <= m))(functools.partial(body, min(m, most)))


def tiles(total, most, act):
    for t in range(0, most, TILE):
        pl.when(total > t)(functools.partial(act, t, min(TILE, most - t)))


def scatter(table_ref, e, o_ref, out_ref, pad):
    at = 0
    for s in range(4):
        out_ref[s, pl.ds(aligned(table_ref[4 + s, e]), pad), :] = o_ref[pl.ds(aligned(at), pad), :]
        at = at + table_ref[s, e]


def combine(table_ref, local, c_ref, out_ref, acc_ref, ps):
    for s, p in enumerate(ps):
        total = table_ref[4 + s, local]
        blocks = (total + (BLOCK - 1)) // BLOCK

        def clear(k, carry, s=s):
            out_ref[s, pl.ds(aligned(k * GROUP), GROUP), :] = jnp.zeros((GROUP, out_ref.shape[2]), BF16)
            return carry

        lax.fori_loop(total // GROUP, blocks * (BLOCK // GROUP), clear, 0)
        acc_ref[...] = jnp.zeros_like(acc_ref)

        def add(k, carry, s=s):
            at = aligned(k * BLOCK, BLOCK)
            acc_ref[...] += dot(c_ref[s, :, pl.ds(at, BLOCK)], out_ref[s, pl.ds(at, BLOCK), :])
            return carry

        lax.fori_loop(0, blocks, add, 0)
        p[...] = acc_ref[...].astype(p.dtype)


def rows_of(table_ref, e):
    return sum(table_ref[s, e] for s in range(4))


def fetch_c(cs, c_ref, c_sem):
    return [pltpu.make_async_copy(c, c_ref.at[s], c_sem.at[s]) for s, c in enumerate(cs)]


def gate_up_kernel(pad, table_ref, z0, z1, z2, z3, c0, c1, c2, c3, wg_ref, wu_ref, wd_ref, h_hbm, p0, p1, p2, p3,
                   seg_ref, z_ref, h_ref, o_ref, out_ref, c_ref, acc_ref, z_sem, h_sem, c_sem):
    e, local = pl.program_id(0), pl.num_programs(0)
    slot, most = lax.rem(e, 2), z_ref.shape[0]

    def segments(e, slot, start):
        for s, z in enumerate((z0, z1, z2, z3)):
            for k in range(pad // PIECE):

                @pl.when(table_ref[s, e] > k * PIECE)
                def _(s=s, z=z, k=k):
                    at = aligned(table_ref[4 + s, e] + k * PIECE)
                    copy = pltpu.make_async_copy(
                        z.at[pl.ds(at, PIECE)], seg_ref.at[slot, s, pl.ds(k * PIECE, PIECE)], z_sem.at[slot, s, k]
                    )
                    copy.start() if start else copy.wait()

    def put(e, slot, start):
        def act(t, size):
            copy = pltpu.make_async_copy(h_ref.at[slot, pl.ds(t, size)], h_hbm.at[e, pl.ds(t, size)], h_sem.at[slot, t // TILE])
            copy.start() if start else copy.wait()

        tiles(rows_of(table_ref, e), most, act)

    @pl.when(e == 0)
    def _():
        segments(e, slot, True)
        for copy in fetch_c((c0, c1, c2, c3), c_ref, c_sem):
            copy.start()

    @pl.when(e + 1 < local)
    def _():
        segments(e + 1, 1 - slot, True)

    segments(e, slot, False)
    at = 0
    for s in range(4):
        z_ref[pl.ds(aligned(at), pad), :] = seg_ref[slot, s]
        at = at + table_ref[s, e]

    @pl.when(e >= 2)
    def _():
        put(e - 2, slot, False)

    def body(m):
        z = z_ref[:m]
        ff = wg_ref.shape[2]
        half = (ff // 2 + 255) // 256 * 256
        for lo, hi in ((0, half), (half, ff)):
            g = dot(z, wg_ref[0, :, lo:hi])
            u = dot(z, wu_ref[0, :, lo:hi])
            h_ref[slot, :m, lo:hi] = (g * jax.nn.sigmoid(g) * u).astype(BF16)
        o_ref[:m] = dot(h_ref[slot, :m, :], wd_ref[0]).astype(BF16)

    by_rows(at, most, body)
    put(e, slot, True)
    scatter(table_ref, e, o_ref, out_ref, pad)

    @pl.when(e == local - 1)
    def _():
        for copy in fetch_c((c0, c1, c2, c3), c_ref, c_sem):
            copy.wait()
        combine(table_ref, local, c_ref, out_ref, acc_ref, (p0, p1, p2, p3))
        put(e - 1, 1 - slot, False)
        put(e, slot, False)


def partial_sums(tokens, width):
    block = pl.BlockSpec((tokens, width), lambda *_: (0, 0), pipeline_mode=pl.Buffered(1))
    return [block] * 4, [jax.ShapeDtypeStruct((tokens, width), t) for t in (F32, BF16, F32, BF16)]


ANY = pl.BlockSpec(memory_space=pl.ANY)


def gate_up(table, zs, cs, w_gate, w_up, w_down, pad, width):
    (experts, d, ff), (tokens, rows), most = w_gate.shape, cs[0].shape, 4 * pad
    specs, shapes = partial_sums(tokens, width)
    return pl.pallas_call(
        functools.partial(gate_up_kernel, pad),
        grid_spec=pltpu.PrefetchScalarGridSpec(
            num_scalar_prefetch=1,
            grid=(experts,),
            in_specs=[ANY] * 8
            + [pl.BlockSpec((1, d, ff), lambda e, *_: (e, 0, 0))] * 2
            + [pl.BlockSpec((1, ff, width), lambda e, *_: (e, 0, 0))],
            out_specs=[ANY] + specs,
            scratch_shapes=[
                pltpu.VMEM((2, 4, pad, d), BF16),
                pltpu.VMEM((most, d), BF16),
                pltpu.VMEM((2, most, ff), BF16),
                pltpu.VMEM((most, width), BF16),
                pltpu.VMEM((4, rows, width), BF16),
                pltpu.VMEM((4, tokens, rows), BF16),
                pltpu.VMEM((tokens, width), F32),
                pltpu.SemaphoreType.DMA((2, 4, pad // PIECE)),
                pltpu.SemaphoreType.DMA((2, (most + TILE - 1) // TILE)),
                pltpu.SemaphoreType.DMA((4,)),
            ],
        ),
        out_shape=[jax.ShapeDtypeStruct((experts, most, ff), BF16)] + shapes,
        compiler_params=params(),
        cost_estimate=cost(4 * experts * most * d * ff, 4 * experts * d * ff),
        name="gate_up",
    )(table, *zs, *cs, w_gate, w_up, w_down)


def down_kernel(pad, table_ref, h_hbm, w_ref, c0, c1, c2, c3, p0, p1, p2, p3,
                h_ref, o_ref, out_ref, c_ref, acc_ref, h_sem, c_sem):
    e, local = pl.program_id(0), pl.num_programs(0)
    slot, most = lax.rem(e, 2), o_ref.shape[0]

    def get(e, slot, start):
        def act(t, size):
            copy = pltpu.make_async_copy(h_hbm.at[e, pl.ds(t, size)], h_ref.at[slot, pl.ds(t, size)], h_sem.at[slot, t // TILE])
            copy.start() if start else copy.wait()

        tiles(rows_of(table_ref, e), most, act)

    @pl.when(e == 0)
    def _():
        get(e, slot, True)
        for copy in fetch_c((c0, c1, c2, c3), c_ref, c_sem):
            copy.start()

    @pl.when(e + 1 < local)
    def _():
        get(e + 1, 1 - slot, True)

    get(e, slot, False)

    def body(m):
        o_ref[:m] = dot(h_ref[slot, :m, :], w_ref[0]).astype(BF16)

    by_rows(rows_of(table_ref, e), most, body)
    scatter(table_ref, e, o_ref, out_ref, pad)

    @pl.when(e == local - 1)
    def _():
        for copy in fetch_c((c0, c1, c2, c3), c_ref, c_sem):
            copy.wait()
        combine(table_ref, local, c_ref, out_ref, acc_ref, (p0, p1, p2, p3))


def down(table, h, w_down, cs, pad, j, width):
    (experts, ff, d), most, (tokens, rows) = w_down.shape, h.shape[1], cs[0].shape
    specs, shapes = partial_sums(tokens, width)
    return pl.pallas_call(
        functools.partial(down_kernel, pad),
        grid_spec=pltpu.PrefetchScalarGridSpec(
            num_scalar_prefetch=1,
            grid=(experts,),
            in_specs=[ANY, pl.BlockSpec((1, ff, width), lambda e, *_: (e, 0, j))] + [ANY] * 4,
            out_specs=specs,
            scratch_shapes=[
                pltpu.VMEM((2, most, ff), BF16),
                pltpu.VMEM((most, width), BF16),
                pltpu.VMEM((4, rows, width), BF16),
                pltpu.VMEM((4, tokens, rows), BF16),
                pltpu.VMEM((tokens, width), F32),
                pltpu.SemaphoreType.DMA((2, (most + TILE - 1) // TILE)),
                pltpu.SemaphoreType.DMA((4,)),
            ],
        ),
        out_shape=shapes,
        compiler_params=params(),
        cost_estimate=cost(2 * width * (experts * most * ff + 4 * rows * tokens), 2 * experts * width * ff),
        name="down",
    )(table, h, w_down, *cs)


def finish_kernel(p_ref, base_ref, q_ref, back_ref, *refs):
    near = p_ref[...] + base_ref[...] + q_ref[...].astype(F32)
    refs[-1][...] = (near + back_ref[...].astype(F32)).astype(BF16)


def finish(p, base, q, back, y, j):
    (tokens, width), d, tile = p.shape, base.shape[1], 256 if p.shape[0] % 256 == 0 else p.shape[0]
    column = pl.BlockSpec((tile, width), lambda i: (i, j))
    own = pl.BlockSpec((tile, width), lambda i: (i, 0))
    return pl.pallas_call(
        finish_kernel,
        grid=(tokens // tile,),
        in_specs=[own, column, own, own] + ([] if y is None else [ANY]),
        out_specs=column,
        out_shape=jax.ShapeDtypeStruct((tokens, d), BF16),
        input_output_aliases={} if y is None else {4: 0},
        cost_estimate=cost(1e9, 1e6),
        name="finish",
    )(p, base, q, back, *([] if y is None else [y]))


def shared_up_kernel(x_ref, g_ref, u_ref, h_ref):
    g = dot(x_ref[...], g_ref[...])
    u = dot(x_ref[...], u_ref[...])
    h_ref[...] = (g * jax.nn.sigmoid(g) * u).astype(BF16)


def shared_up(x, s_gate, s_up, tile=256):
    (tokens, d), ff = x.shape, s_gate.shape[1]
    return pl.pallas_call(
        shared_up_kernel,
        grid=(ff // tile,),
        in_specs=[whole(x)] + [pl.BlockSpec((d, tile), lambda k: (0, k))] * 2,
        out_specs=pl.BlockSpec((tokens, tile), lambda k: (0, k)),
        out_shape=jax.ShapeDtypeStruct((tokens, ff), BF16),
        compiler_params=params(),
        cost_estimate=cost(4 * tokens * d * ff, 4 * d * ff),
        name="shared_up",
    )(x, s_gate, s_up)


def shared_down_kernel(h_ref, d_ref, y_ref):
    y_ref[...] = dot(h_ref[...], d_ref[...])


def shared_down(h, s_down, tile=512):
    (tokens, ff), d = h.shape, s_down.shape[1]
    return pl.pallas_call(
        shared_down_kernel,
        grid=(d // tile,),
        in_specs=[whole(h), pl.BlockSpec((ff, tile), lambda k: (0, k))],
        out_specs=pl.BlockSpec((tokens, tile), lambda k: (0, k)),
        out_shape=jax.ShapeDtypeStruct((tokens, d), F32),
        compiler_params=params(),
        cost_estimate=cost(2 * tokens * d * ff, 2 * d * ff),
        name="shared_down",
    )(h, s_down)


def solution(mesh):
    members = mesh.shape["ep"]

    def send(v, flip):
        return lax.ppermute(v, "ep", [(i, i ^ flip) for i in range(members)])

    def step(x, expert, slot, gate, w_gate, w_up, w_down, s_gate, s_up, s_down):
        tokens, d = x.shape[2:]
        top, local = expert.shape[3], w_gate.shape[0]
        slots = 5 * tokens * top // (4 * local * members)
        pad = (slots + PIECE - 1) // PIECE * PIECE
        rows = (local * pad + BLOCK - 1) // BLOCK * BLOCK
        x, expert, slot, gate = (v.reshape(v.shape[2:]) for v in (x, expert, slot, gate))
        me = lax.axis_index("ep").astype(I32).reshape(1)

        x2 = send(x, 2)
        code = jnp.where(slot < slots, expert * STRIDE + slot, -1)
        info = jnp.concatenate([code.T.astype(F32), gate.T])
        infos = [info] + [send(info, f) for f in (1, 2, 3)]
        x1 = send(x, 1)
        pos, table = route(me, infos, local, top)
        hs = shared_up(x, s_gate, s_up)
        base = shared_down(hs, s_down)
        zs, cs = [], []
        x3 = send(x2, 1)
        for s, v in enumerate((x, x1, x2, x3)):
            z, c = gather(table, pos, infos[s], v, rows, s, local)
            zs.append(z)
            cs.append(c)
        width, y = d // CHUNKS, None
        h, *ps = gate_up(table, zs, cs, w_gate, w_up, w_down, pad, width)
        parts = []
        for j in range(CHUNKS):
            if j:
                ps = down(table, h, w_down, cs, pad, j, width)
            p0, p1, p2, p3 = ps
            q3 = send(p3, 1)
            back = send((p2 + q3.astype(F32)).astype(BF16), 2)
            q1 = send(p1, 1)
            parts.append((p0, q1, back))
        for j, (p0, q1, back) in enumerate(parts):
            y = finish(p0, base, q1, back, y, j)
        return y.reshape(1, 1, tokens, d)

    data = P("dp", "ep", None, None)
    w, s = P("ep", None, None), P(None, None)
    return jax.shard_map(step, mesh=mesh, in_specs=(data,) * 4 + (w,) * 3 + (s,) * 3, out_specs=data, check_vma=False)
```

```python
import functools

import jax
import jax.numpy as jnp
from jax import lax
from jax.experimental import pallas as pl
from jax.experimental.pallas import tpu as pltpu
from jax.sharding import PartitionSpec as P


F32, BF16, I32 = jnp.float32, jnp.bfloat16, jnp.int32
VMEM = 66_000_000
GROUP, BLOCK, STRIDE, TILE = 16, 256, 128, 128
WIDTHS = (10, 6)


def dot(a, b):
    return jnp.dot(a, b, preferred_element_type=F32)


def params():
    return pltpu.CompilerParams(vmem_limit_bytes=VMEM)


def cost(flops, nbytes):
    return pl.CostEstimate(flops=int(flops), bytes_accessed=int(nbytes), transcendentals=0)


def whole(v):
    return pl.BlockSpec(v.shape, lambda *_: (0,) * v.ndim, pipeline_mode=pl.Buffered(1))


def aligned(v, m=GROUP):
    return pl.multiple_of(v, m)


def route_kernel(local, me_ref, *refs):
    infos, (pos_ref, weight_ref, table_ref) = refs[:4], refs[4:]
    tokens, top = infos[0].shape[1], infos[0].shape[0] // 2
    expert = lax.broadcasted_iota(I32, (local, tokens), 0)
    a = lax.broadcasted_iota(I32, (local, STRIDE), 0)
    b = lax.broadcasted_iota(I32, (local, STRIDE), 1)
    for s, info in enumerate(infos):
        code = info[:top, :].astype(I32) - me_ref[0] * (local * STRIDE)
        mine = (code >= 0) & (code < local * STRIDE)
        which = jnp.where(mine, lax.shift_right_logical(code, 7), -1)
        place = jnp.where(mine, code & (STRIDE - 1), 0)
        most = jnp.zeros((local, tokens), I32)
        for j in range(top):
            most = jnp.maximum(most, jnp.where(which[j : j + 1] == expert, place[j : j + 1] + 1, 0))
        used = jnp.max(most.astype(F32), axis=1, keepdims=True).astype(I32)
        used = (used + (GROUP - 1)) & ~(GROUP - 1)
        as_row = lambda m: jnp.sum(jnp.where(m, used.astype(F32), 0.0), axis=0, keepdims=True)
        row, start_row = as_row(a == b), as_row(a < b)
        start = jnp.sum(jnp.where((b < a) & (b < local), row, 0.0), axis=1, keepdims=True).astype(I32)
        for j in range(top):
            at = jnp.sum(jnp.where(which[j : j + 1] == expert, start, 0).astype(F32), axis=0, keepdims=True).astype(I32)
            pos_ref[s, j : j + 1, :] = jnp.where(mine[j : j + 1], at + place[j : j + 1], -1)
        weight_ref[s] = info[top:, :]
        table_ref[s : s + 1, :] = row.astype(I32)
        table_ref[4 + s : 5 + s, :] = start_row.astype(I32)


def route(me, infos, local):
    top, tokens = infos[0].shape[0] // 2, infos[0].shape[1]
    return pl.pallas_call(
        functools.partial(route_kernel, local),
        in_specs=[pl.BlockSpec(memory_space=pltpu.SMEM)] + [pl.BlockSpec(memory_space=pltpu.VMEM)] * 4,
        out_specs=[pl.BlockSpec(memory_space=pltpu.VMEM)] * 3,
        out_shape=[
            jax.ShapeDtypeStruct((4, top, tokens), I32),
            jax.ShapeDtypeStruct((4, top, tokens), F32),
            jax.ShapeDtypeStruct((8, STRIDE), I32),
        ],
        cost_estimate=cost(1e9, 1e6),
        name="route",
    )(me, *infos)


def select_kernel(local, table_ref, pos_ref, weight_ref, one_ref, c_ref):
    s, i, (top, tokens) = pl.program_id(0), pl.program_id(1), pos_ref.shape[1:]

    @pl.when(i * BLOCK < table_ref[4 + s, local])
    def _():
        row = lax.broadcasted_iota(I32, (BLOCK, tokens), 0) + i * BLOCK
        c = jnp.full((BLOCK, tokens), jnp.inf, F32)
        for j in range(top):
            c = jnp.where(pos_ref[0, j : j + 1, :] == row, weight_ref[0, j : j + 1, :], c)
        empty = c == jnp.inf
        one_ref[0] = jnp.where(empty, 0.0, 1.0).astype(BF16)
        c_ref[0] = jnp.where(empty, 0.0, c).astype(BF16).T


def last_block(i, t, s, local):
    return jnp.minimum(i, jnp.maximum((t[4 + s, local] + (BLOCK - 1)) // BLOCK - 1, 0))


def select(table, pos, weight, rows, local):
    sources, _, tokens = pos.shape
    own = lambda v: pl.BlockSpec((1, *v.shape[1:]), lambda s, i, t: (s, 0, 0))
    return pl.pallas_call(
        functools.partial(select_kernel, local),
        grid_spec=pltpu.PrefetchScalarGridSpec(
            num_scalar_prefetch=1,
            grid=(sources, rows // BLOCK),
            in_specs=[own(pos), own(weight)],
            out_specs=[
                pl.BlockSpec((1, BLOCK, tokens), lambda s, i, t: (s, last_block(i, t, s, local), 0)),
                pl.BlockSpec((1, tokens, BLOCK), lambda s, i, t: (s, 0, last_block(i, t, s, local))),
            ],
        ),
        out_shape=[
            jax.ShapeDtypeStruct((sources, rows, tokens), BF16),
            jax.ShapeDtypeStruct((sources, tokens, rows), BF16),
        ],
        compiler_params=params(),
        cost_estimate=cost(1e10, 4 * sources * rows * tokens),
        name="select",
    )(table, pos, weight)


def gather_kernel(first, local, table_ref, one_ref, *refs):
    xs, z_ref = refs[:-1], refs[-1]
    s, i = pl.program_id(0), pl.program_id(1)
    for k, x_ref in enumerate(xs):

        @pl.when((s == k) & (i * BLOCK < table_ref[4 + first + k, local]))
        def _(x_ref=x_ref):
            z_ref[0] = dot(one_ref[0], x_ref[...]).astype(BF16)


def gather(table, one, xs, first, local):
    (tokens, d), rows = xs[0].shape, one.shape[1]
    return pl.pallas_call(
        functools.partial(gather_kernel, first, local),
        grid_spec=pltpu.PrefetchScalarGridSpec(
            num_scalar_prefetch=1,
            grid=(len(xs), rows // BLOCK),
            in_specs=[
                pl.BlockSpec((1, BLOCK, tokens), lambda s, i, t: (first + s, last_block(i, t, first + s, local), 0)),
                *map(whole, xs),
            ],
            out_specs=pl.BlockSpec((1, BLOCK, d), lambda s, i, t: (s, last_block(i, t, first + s, local), 0)),
        ),
        out_shape=jax.ShapeDtypeStruct((len(xs), rows, d), BF16),
        compiler_params=params(),
        cost_estimate=cost(2 * len(xs) * rows * tokens * d, 2 * len(xs) * rows * (tokens + d)),
        name="gather",
    )(table, one, *xs)


def by_rows(total, most, body, step=64):
    below = 0
    for m in [*range(TILE, most, step), most]:
        pl.when((total > below) & (total <= m))(functools.partial(body, m))
        below = m


def rows_of(table_ref, e):
    return sum(table_ref[s, e] for s in range(4))


def go(copy, start):
    copy.start() if start else copy.wait()


def exact(used, most, act):
    k, size = 0, GROUP
    while size <= most:
        pl.when((used & size) > 0)(functools.partial(act, k, used & ~(2 * size - 1), size))
        k, size = k + 1, 2 * size


def gate_up_kernel(pad, table_ref, z01, z2, one_hbm, x_hbm, wg_hbm, wu_hbm, h_hbm,
                   z_ref, h_ref, one_ref, x_ref, far_ref, wg_ref, wu_ref, z_sem, h_sem, x_sem, w_sem):
    e, local = pl.program_id(0), pl.num_programs(0)
    most, depth = z_ref.shape[1], wg_ref.shape[0]
    slot = lax.rem(e, depth)
    total = table_ref[7, wg_hbm.shape[0]]

    def weights(e, start):
        at = lax.rem(e, depth)
        go(pltpu.make_async_copy(wg_hbm.at[e], wg_ref.at[at], w_sem.at[at, 0]), start)
        go(pltpu.make_async_copy(wu_hbm.at[e], wu_ref.at[at], w_sem.at[at, 1]), start)

    def segments(e, start):
        slot, first = lax.rem(e, depth), 0
        for s, z in enumerate((z01.at[0], z01.at[1], z2.at[0])):

            def act(k, skip, size, s=s, z=z, first=first):
                source, target = aligned(table_ref[4 + s, e] + skip), aligned(first + skip)
                go(pltpu.make_async_copy(
                    z.at[pl.ds(source, size)], z_ref.at[slot, pl.ds(target, size)], z_sem.at[slot, s, k]
                ), start)

            exact(table_ref[s, e], pad, act)
            first = first + table_ref[s, e]

    def put(e, start):
        slot = lax.rem(e, depth)

        def act(k, skip, size):
            rows = pl.ds(aligned(skip), size)
            go(pltpu.make_async_copy(h_ref.at[slot, rows], h_hbm.at[e, rows], h_sem.at[slot, k]), start)

        exact(rows_of(table_ref, e), most, act)

    @pl.when(e == 0)
    def _():
        fetch = [pltpu.make_async_copy(x_hbm, x_ref, x_sem.at[0]), pltpu.make_async_copy(one_hbm.at[3], one_ref, x_sem.at[1])]
        for copy in fetch:
            copy.start()
        for k in range(depth):
            segments(k, True)
            weights(k, True)
        for copy in fetch:
            copy.wait()

        def block(k, carry):
            at = aligned(k * BLOCK, BLOCK)
            far_ref[pl.ds(at, BLOCK), :] = dot(one_ref[pl.ds(at, BLOCK), :], x_ref[...]).astype(BF16)
            return carry

        lax.fori_loop(0, (total + (BLOCK - 1)) // BLOCK, block, 0)

    segments(e, False)
    at = table_ref[0, e] + table_ref[1, e] + table_ref[2, e]
    z_ref[slot, pl.ds(aligned(at), pad), :] = far_ref[pl.ds(aligned(table_ref[7, e]), pad), :]

    @pl.when(e >= depth)
    def _():
        put(e - depth, False)

    weights(e, False)

    def body(m):
        z, ff = z_ref[slot, :m, :], wg_ref.shape[2]
        full, half = ff // 256 * 256, ff // 512 * 256 + 256
        for lo, hi in ((0, half), (half, full)):
            g = dot(z, wg_ref[slot, :, lo:hi])
            u = dot(z, wu_ref[slot, :, lo:hi])
            h_ref[slot, :m, lo:hi] = (g * jax.nn.sigmoid(g) * u).astype(BF16)
        if full < ff:
            both = dot(z, jnp.concatenate([wg_ref[slot, :, full:], wu_ref[slot, :, full:]], axis=1))
            g, u = both[:, : ff - full], both[:, ff - full :]
            h_ref[slot, :m, full:] = (g * jax.nn.sigmoid(g) * u).astype(BF16)

    by_rows(rows_of(table_ref, e), most, body)
    put(e, True)

    @pl.when(e + depth < local)
    def _():
        segments(e + depth, True)
        weights(e + depth, True)

    @pl.when(e == local - 1)
    def _():
        for k in range(depth):
            put(e - k, False)


ANY = pl.BlockSpec(memory_space=pl.ANY)


def gate_up(table, zs, one, x, w_gate, w_up, pad):
    (experts, d, ff), (_, rows, tokens), most, depth = w_gate.shape, one.shape, 4 * pad, 3
    return pl.pallas_call(
        functools.partial(gate_up_kernel, pad),
        grid_spec=pltpu.PrefetchScalarGridSpec(
            num_scalar_prefetch=1,
            grid=(experts,),
            in_specs=[ANY] * 6,
            out_specs=ANY,
            scratch_shapes=[
                pltpu.VMEM((depth, most, d), BF16),
                pltpu.VMEM((depth, most, ff), BF16),
                pltpu.VMEM((rows, tokens), BF16),
                pltpu.VMEM((tokens, d), BF16),
                pltpu.VMEM((rows, d), BF16),
                pltpu.VMEM((depth, d, ff), BF16),
                pltpu.VMEM((depth, d, ff), BF16),
                pltpu.SemaphoreType.DMA((depth, 3, 8)),
                pltpu.SemaphoreType.DMA((depth, 8)),
                pltpu.SemaphoreType.DMA((2,)),
                pltpu.SemaphoreType.DMA((depth, 2)),
            ],
        ),
        out_shape=jax.ShapeDtypeStruct((experts, most, ff), BF16),
        compiler_params=params(),
        cost_estimate=cost(4 * experts * most * d * ff, 4 * experts * d * ff),
        name="gate_up",
    )(table, *zs, one, x, w_gate, w_up)


def down_kernel(pad, sources, first, table_ref, h_hbm, w_hbm, c_hbm, *refs):
    e, local = pl.program_id(0), pl.num_programs(0)
    outs, (h_ref, w_ref, o_ref, out_ref, c_ref, acc_ref, h_sem, w_sem, c_sem) = refs[: len(sources)], refs[len(sources) :]
    (depth, most, _), experts, width = h_ref.shape, w_hbm.shape[0], w_ref.shape[2]
    sums = [acc_ref.at[i // 2] if i % 2 else outs[i] for i in range(len(sources))]
    used = lambda e: sum(table_ref[s, e] for s in sources)

    def get(e, start):
        at = lax.rem(e, depth)
        before = sum(table_ref[s, e] for s in range(sources[0]))

        def act(k, skip, size):
            go(pltpu.make_async_copy(
                h_hbm.at[e, pl.ds(aligned(before + skip), size)],
                h_ref.at[at, pl.ds(aligned(skip), size)],
                h_sem.at[at, k],
            ), start)

        exact(used(e), most, act)
        go(pltpu.make_async_copy(w_hbm.at[e, :, pl.ds(first, width)], w_ref.at[at], w_sem.at[at]), start)

    def get_c(i, k):
        columns = pl.ds(aligned(k * BLOCK, BLOCK), BLOCK)
        return pltpu.make_async_copy(c_hbm.at[sources[i], :, columns], c_ref.at[i, :, columns], c_sem.at[i, k])

    def add(i, k):
        get_c(i, k).wait()
        at = aligned(k * BLOCK, BLOCK)
        sums[i][...] += dot(c_ref[i, :, pl.ds(at, BLOCK)], out_ref[i, pl.ds(at, BLOCK), :])

    @pl.when(e == 0)
    def _():
        get(0, True)
        get(1, True)
        for k in range(c_ref.shape[2] // BLOCK):
            for i, s in enumerate(sources):
                pl.when(table_ref[4 + s, experts] > k * BLOCK)(lambda i=i, k=k: get_c(i, k).start())
        for k in range(2, depth):
            get(k, True)
        for v in sums:
            v[...] = jnp.zeros_like(v)

    get(e, False)
    ring = lax.rem(e, depth)

    def body(m):
        o_ref[:m] = dot(h_ref[ring, :m, :], w_ref[ring]).astype(BF16)

    by_rows(used(e), most, body, TILE)

    @pl.when(e + depth < local)
    def _():
        get(e + depth, True)

    at = 0
    for i, s in enumerate(sources):
        out_ref[i, pl.ds(aligned(table_ref[4 + s, e]), pad), :] = o_ref[pl.ds(aligned(at), pad), :]
        at = at + table_ref[s, e]
    for i, s in enumerate(sources):
        before = table_ref[4 + s, e]
        k = before // BLOCK
        pl.when((before + table_ref[s, e]) // BLOCK > k)(lambda i=i, k=k: add(i, k))

    @pl.when(e == local - 1)
    def _():
        for i, s in enumerate(sources):
            total = table_ref[4 + s, experts]

            @pl.when(lax.rem(total, BLOCK) > 0)
            def _(i=i, total=total):
                def clear(k, carry):
                    out_ref[i, pl.ds(aligned(k * GROUP), GROUP), :] = jnp.zeros((GROUP, width), BF16)
                    return carry

                lax.fori_loop(total // GROUP, (total // BLOCK + 1) * (BLOCK // GROUP), clear, 0)
                add(i, total // BLOCK)

        for i in range(1, len(sources), 2):
            outs[i][...] = sums[i][...].astype(BF16)


def down(table, h, w_down, c, pad, sources, first, width):
    (experts, ff, d), (_, tokens, rows), most, n = w_down.shape, c.shape, len(sources) * pad, len(sources)
    depth = 6 if width * n <= 2048 else 5
    block = pl.BlockSpec((tokens, width), lambda *_: (0, 0), pipeline_mode=pl.Buffered(1))
    return pl.pallas_call(
        functools.partial(down_kernel, pad, sources, first),
        grid_spec=pltpu.PrefetchScalarGridSpec(
            num_scalar_prefetch=1,
            grid=(experts,),
            in_specs=[ANY] * 3,
            out_specs=[block] * n,
            scratch_shapes=[
                pltpu.VMEM((depth, most, ff), BF16),
                pltpu.VMEM((depth, ff, width), BF16),
                pltpu.VMEM((most, width), BF16),
                pltpu.VMEM((n, rows, width), BF16),
                pltpu.VMEM((n, tokens, rows), BF16),
                pltpu.VMEM((n // 2, tokens, width), F32),
                pltpu.SemaphoreType.DMA((depth, 8)),
                pltpu.SemaphoreType.DMA((depth,)),
                pltpu.SemaphoreType.DMA((n, rows // BLOCK)),
            ],
        ),
        out_shape=[jax.ShapeDtypeStruct((tokens, width), (F32, BF16)[s % 2]) for s in sources],
        compiler_params=params(),
        cost_estimate=cost(2 * width * (experts * most * ff + n * rows * tokens), 2 * experts * width * ff),
        name="down",
    )(table, h, w_down, c)


def finish_kernel(p_ref, base_ref, q_ref, back_ref, *refs):
    near = p_ref[...] + base_ref[...] + q_ref[...].astype(F32)
    refs[-1][...] = (near + back_ref[...].astype(F32)).astype(BF16)


def finish(p, base, q, back, y, first):
    (tokens, width), d, unit = p.shape, base.shape[1], 256
    own = pl.BlockSpec((tokens, unit), lambda i: (0, i))
    column = pl.BlockSpec((tokens, unit), lambda i: (0, first // unit + i))
    return pl.pallas_call(
        finish_kernel,
        grid=(width // unit,),
        in_specs=[own, column, own, own] + ([] if y is None else [ANY]),
        out_specs=column,
        out_shape=jax.ShapeDtypeStruct((tokens, d), BF16),
        input_output_aliases={} if y is None else {4: 0},
        cost_estimate=cost(1e9, 1e6),
        name="finish",
    )(p, base, q, back, *([] if y is None else [y]))


def shared_kernel(up_steps, x_ref, g_ref, u_ref, d_ref, y_ref, h_ref):
    k, tile = pl.program_id(0), g_ref.shape[1]

    @pl.when(k < up_steps)
    def _():
        g = dot(x_ref[...], g_ref[...])
        u = dot(x_ref[...], u_ref[...])
        h_ref[:, pl.ds(aligned(k * tile, tile), tile)] = (g * jax.nn.sigmoid(g) * u).astype(BF16)

    @pl.when(k >= up_steps)
    def _():
        y_ref[...] = dot(h_ref[...], d_ref[...])


def shared(x, s_gate, s_up, s_down, up=256, out=512):
    (tokens, d), ff = x.shape, s_gate.shape[1]
    steps = ff // up
    return pl.pallas_call(
        functools.partial(shared_kernel, steps),
        grid=(steps + d // out,),
        in_specs=[whole(x)]
        + [pl.BlockSpec((d, up), lambda k: (0, jnp.minimum(k, steps - 1)))] * 2
        + [pl.BlockSpec((ff, out), lambda k: (0, jnp.maximum(k - steps, 0)))],
        out_specs=pl.BlockSpec((tokens, out), lambda k: (0, jnp.maximum(k - steps, 0))),
        out_shape=jax.ShapeDtypeStruct((tokens, d), F32),
        scratch_shapes=[pltpu.VMEM((tokens, ff), BF16)],
        compiler_params=params(),
        cost_estimate=cost(6 * tokens * d * ff, 6 * d * ff),
        name="shared",
    )(x, s_gate, s_up, s_down)


def solution(mesh):
    members = mesh.shape["ep"]

    def send(v, flip):
        return lax.ppermute(v, "ep", [(i, i ^ flip) for i in range(members)])

    def step(x, expert, slot, gate, w_gate, w_up, w_down, s_gate, s_up, s_down):
        tokens, d = x.shape[2:]
        top, local = expert.shape[3], w_gate.shape[0]
        slots = 5 * tokens * top // (4 * local * members)
        pad = (slots + GROUP - 1) // GROUP * GROUP
        rows = (local * pad + BLOCK - 1) // BLOCK * BLOCK
        x, expert, slot, gate = (v.reshape(v.shape[2:]) for v in (x, expert, slot, gate))
        me = lax.axis_index("ep").astype(I32).reshape(1)

        x2 = send(x, 2)
        code = jnp.where(slot < slots, expert * STRIDE + slot, -1)
        info = jnp.concatenate([code.T.astype(F32), gate.T])
        infos = [info] + [send(info, f) for f in (1, 2, 3)]
        x1 = send(x, 1)
        pos, weight, table = route(me, infos, local)
        base = shared(x, s_gate, s_up, s_down)
        one, c = select(table, pos, weight, rows, local)
        x3 = send(x2, 1)
        z01 = gather(table, one, (x, x1), 0, local)
        z2 = gather(table, one, (x2,), 2, local)
        h = gate_up(table, (z01, z2), one, x3, w_gate, w_up, pad)
        widths = [d * v // 16 for v in WIDTHS]
        columns = [(sum(widths[:j]), v) for j, v in enumerate(widths)]
        back, near, y = [], [], None
        last = len(columns) - 1
        for j, (first, width) in enumerate(columns):
            sources = (0, 1, 2, 3) if j == last else (2, 3)
            *both, p2, p3 = down(table, h, w_down, c, pad, sources, first, width)
            q3 = send(p3, 1)
            back.append(send((p2 + q3.astype(F32)).astype(BF16), 2))
        for j, (first, width) in enumerate(columns):
            p0, p1 = both if j == last else down(table, h, w_down, c, pad, (0, 1), first, width)
            near.append((p0, send(p1, 1)))
        for j, (first, width) in reversed([*enumerate(columns)]):
            y = finish(near[j][0], base, near[j][1], back[j], y, first)
        return y.reshape(1, 1, tokens, d)

    data = P("dp", "ep", None, None)
    w, s = P("ep", None, None), P(None, None)
    return jax.shard_map(step, mesh=mesh, in_specs=(data,) * 4 + (w,) * 3 + (s,) * 3, out_specs=data, check_vma=False)
```
